32 devices in a mesh: rep: 2 (over x), dp: 16 (over y, z, core).
Axes of the slice: x: 2, y: 2, z: 4, core: 2. Of those that a mesh axis runs over, the one named last changes fastest.
Arguments:
- a: bfloat16 [32, 4, 4096, 1280], P(('rep', 'dp')), parts along dimension 0
- g: bfloat16 [32, 4, 4096, 5120], P(('rep', 'dp')), parts along dimension 0
Outputs:
- output: bfloat16 [8, 1280, 5120], P('rep'), parts along dimension 0
There are 2 independent parts. The reference program is written for one: setup_inputs(seed, part) draws one part's arguments, and reference() takes and returns one part's arrays. A program takes and returns all parts, laid end to end along the dimension named above; each array names one.
All inputs are finite; a program needn't handle non-finite values.
Results may differ from the reference program's by a relative error of at most 0.012.
Values are sent between devices in bfloat16 or wider.
A program may use at most 2 GiB of HBM per device.

```python
import jax
import jax.numpy as jnp
from jax import lax

DEVICES = 16
MATRICES = 4
TOKENS = 4096
D = 1280
FF = 5120


def setup_inputs(seed: int = 0, part: int = 0) -> dict:
    ka, kg, ks = (jax.random.fold_in(k, part) for k in jax.random.split(jax.random.key(seed), 3))
    size = 2.0 ** jax.random.uniform(ks, (DEVICES, MATRICES, 1, 1), jnp.float32, -1.0, 1.0)
    a = jax.random.normal(ka, (DEVICES, MATRICES, TOKENS, D), jnp.float32)
    g = size * jax.random.normal(kg, (DEVICES, MATRICES, TOKENS, FF), jnp.float32) * (DEVICES * TOKENS) ** -0.5
    return {"a": a.astype(jnp.bfloat16), "g": g.astype(jnp.bfloat16)}


def reference(a, g):
    def take(so_far, one):
        return so_far + jnp.einsum("ntd,ntf->ndf", *one, preferred_element_type=jnp.float32), None

    return lax.scan(take, jnp.zeros((MATRICES, D, FF), jnp.float32), (a, g))[0].astype(jnp.bfloat16)
```

```python
import jax
import jax.numpy as jnp
from jax import lax
from jax.experimental import pallas as pl
from jax.experimental.pallas import tpu as pltpu
from jax.sharding import PartitionSpec as P

MESH = pl.DeviceIdType.MESH
CHIPS_Z = 4
LEFT, RIGHT, ACROSS, PAIR = range(4)

SPLIT = 2
COLS = 256
A_STEP = 256
LAG0 = 2
LAG = 3
STAGES = 8
RING = LAG0 + LAG * STAGES + 3
SUMS = LAG0 + LAG * (STAGES // 2) + 1


def flag(condition):
    return jnp.where(condition, jnp.int32(1), jnp.int32(0))


def role(unit, y, z):
    turn = lax.rem(unit, jnp.int32(10))
    half = turn // 5
    kind = turn - 5 * half
    across_first = kind < 3
    odd = lax.rem(turn, jnp.int32(2))
    root_z = jnp.where(across_first, 1 + odd, 2 * half + kind - 3)
    root_y = jnp.where(across_first, lax.rem(turn // 2, jnp.int32(2)), odd)
    below, above, same = z < root_z, z > root_z, z == root_z
    home = y == root_y
    far = 3 - z
    height = jnp.maximum(root_z, 3 - root_z) + 1
    along = jnp.where(below, z, far)
    level = jnp.where(
        across_first,
        jnp.where(home, jnp.where(same, height, 1 + along), 0),
        jnp.where(same, jnp.where(home, height, height - 1), along),
    )
    depth = jnp.abs(z - root_z) + flag(~home)
    in_line = home | ~across_first
    return dict(
        level=level,
        down=height + depth,
        root=home & same,
        up_right=in_line & below,
        up_left=in_line & above,
        up_across=~home & (across_first | same),
        from_left=in_line & (z <= root_z) & (z > 0),
        from_right=in_line & (z >= root_z) & (z < CHIPS_Z - 1),
        from_across=home & (across_first | same),
    )


def kernel(
    a_hbm, g_hbm, out_hbm,
    a_t, a_in, g_in, product, sums, outgoing, arrived, final,
    a_sem, g_sem, outgoing_sem, arrived_sem, climb_sem, final_sem, leave_sem, other_sem,
):
    matrices, tokens, d = a_hbm.shape
    ff = g_hbm.shape[2]
    rows = d // (2 * SPLIT)
    blocks = ff // COLS
    steps = blocks * SPLIT
    units = matrices * steps
    chunks = tokens // A_STEP

    rep, me = lax.axis_index("rep"), lax.axis_index("dp")
    core = lax.rem(me, 2)
    chip = me // 2
    z = lax.rem(chip, CHIPS_Z)
    y = chip // CHIPS_Z
    partner = me + 1 - 2 * core
    across = me + 2 * CHIPS_Z * (1 - 2 * y)

    def device(i):
        return (rep, i)

    barrier = pltpu.get_barrier_semaphore()

    def greet(i):
        pl.semaphore_signal(barrier, inc=1, device_id=device(i), device_id_type=MESH)

    greet(partner)
    greet(across)

    @pl.when(z > 0)
    def _():
        greet(me - 2)

    @pl.when(z < CHIPS_Z - 1)
    def _():
        greet(me + 2)

    def a_copy(n, i, slot):
        return pltpu.make_async_copy(
            a_hbm.at[n, pl.ds(pl.multiple_of(i * A_STEP, A_STEP), A_STEP)], a_in.at[slot], a_sem.at[slot]
        )

    def g_copy(tile):
        n = tile // blocks
        column = pl.multiple_of((tile - n * blocks) * COLS, COLS)
        slot = lax.rem(tile, 3)
        return pltpu.make_async_copy(g_hbm.at[n, :, pl.ds(column, COLS)], g_in.at[slot], g_sem.at[slot])

    def transpose(n, i, slot):
        a_t[lax.rem(n, 2), :, pl.ds(pl.multiple_of(i * A_STEP, A_STEP), A_STEP)] = a_in[slot].T

    def place(unit, of_core):
        tile = unit // SPLIT
        n = tile // blocks
        row = pl.multiple_of((unit - tile * SPLIT) * (2 * rows) + of_core * rows, rows)
        column = pl.multiple_of((tile - n * blocks) * COLS, COLS)
        return out_hbm.at[n, pl.ds(row, rows), pl.ds(column, COLS)]

    def slot_of(unit):
        return lax.rem(unit, RING)

    def pair_copy(unit):
        slot = slot_of(unit)
        return pltpu.make_async_remote_copy(
            src_ref=outgoing.at[slot], dst_ref=arrived.at[PAIR, slot],
            send_sem=outgoing_sem.at[slot], recv_sem=arrived_sem.at[PAIR, slot],
            device_id=device(partner), device_id_type=MESH,
        )

    def climb_copy(unit, side, to):
        slot = slot_of(unit)
        return pltpu.make_async_remote_copy(
            src_ref=arrived.at[PAIR, slot], dst_ref=arrived.at[side, slot],
            send_sem=climb_sem.at[slot], recv_sem=arrived_sem.at[side, slot],
            device_id=device(to), device_id_type=MESH,
        )

    def final_copy(unit, side, to):
        slot = slot_of(unit)
        return pltpu.make_async_remote_copy(
            src_ref=final.at[slot], dst_ref=final.at[slot],
            send_sem=leave_sem.at[side, slot], recv_sem=final_sem.at[slot],
            device_id=device(to), device_id_type=MESH,
        )

    def other_copy(unit, of_core):
        slot = slot_of(unit)
        return pltpu.make_async_remote_copy(
            src_ref=final.at[slot], dst_ref=place(unit, of_core),
            send_sem=leave_sem.at[PAIR, slot], recv_sem=other_sem.at[slot],
            device_id=device(partner), device_id_type=MESH,
        )

    def own_copy(unit):
        slot = slot_of(unit)
        return pltpu.make_async_copy(final.at[slot], place(unit, core), leave_sem.at[4, slot])

    def compute(unit):
        tile = unit // SPLIT
        part = unit - tile * SPLIT
        n = tile // blocks
        step = unit - n * steps

        @pl.when(part == 0)
        def _():
            @pl.when(tile + 2 < matrices * blocks)
            def _():
                g_copy(tile + 2).start()

            g_copy(tile).wait()

        left = a_t[lax.rem(n, 2), pl.ds(pl.multiple_of(part * 2 * rows, 2 * rows), 2 * rows), :]
        product[...] = jnp.dot(left, g_in[lax.rem(tile, 3)], preferred_element_type=jnp.float32)
        slot = slot_of(unit)
        outgoing[slot] = product[pl.ds(pl.multiple_of((1 - core) * rows, rows), rows), :].astype(jnp.bfloat16)
        pair_copy(unit).start()
        sums[lax.rem(unit, SUMS)] = product[pl.ds(pl.multiple_of(core * rows, rows), rows), :]

        @pl.when(n < matrices - 1)
        def _():
            @pl.when(step < chunks)
            def _():
                a_copy(n + 1, step, lax.rem(step, 2)).start()

            @pl.when((step >= 1) & (step <= chunks))
            def _():
                i = step - 1
                a_copy(n + 1, i, lax.rem(i, 2)).wait()
                transpose(n + 1, i, lax.rem(i, 2))

    def climb(unit, r):
        slot = slot_of(unit)
        at = lax.rem(unit, SUMS)
        for side, there, source in (
            (LEFT, r["from_left"], me - 2),
            (RIGHT, r["from_right"], me + 2),
            (ACROSS, r["from_across"], across),
        ):
            @pl.when(there)
            def _():
                climb_copy(unit, side, source).wait_recv()
                sums[at] = sums[at] + arrived[side, slot].astype(jnp.float32)

        pair_copy(unit).wait_recv()
        total = (sums[at] + arrived[PAIR, slot].astype(jnp.float32)).astype(jnp.bfloat16)

        @pl.when(r["root"])
        def _():
            final[slot] = total

        @pl.when(~r["root"])
        def _():
            arrived[PAIR, slot] = total

        for side, there, to in (
            (LEFT, r["up_right"], me + 2),
            (RIGHT, r["up_left"], me - 2),
            (ACROSS, r["up_across"], across),
        ):
            @pl.when(there)
            def _():
                climb_copy(unit, side, to).start()

    def children(unit, r, act):
        for side, there, to in (
            (LEFT, r["from_left"], me - 2),
            (RIGHT, r["from_right"], me + 2),
            (ACROSS, r["from_across"], across),
        ):
            @pl.when(there)
            def _():
                act(final_copy(unit, side, to))

    def descend(unit, r):
        @pl.when(~r["root"])
        def _():
            climb_copy(unit, LEFT, partner).wait_send()
            final_copy(unit, LEFT, partner).wait_recv()

        children(unit, r, lambda copy: copy.start())
        other_copy(unit, core).start()
        own_copy(unit).start()

    def retire(unit):
        r = role(unit, y, z)
        pair_copy(unit).wait_send()
        children(unit, r, lambda copy: copy.wait_send())
        other_copy(unit, core).wait_send()
        own_copy(unit).wait()
        other_copy(unit, 1 - core).wait_recv()

    a_copy(0, 0, 0).start()
    g_copy(0).start()
    g_copy(1).start()

    def first(i, carry):
        @pl.when(i + 1 < chunks)
        def _():
            a_copy(0, i + 1, lax.rem(i + 1, 2)).start()

        a_copy(0, i, lax.rem(i, 2)).wait()
        transpose(0, i, lax.rem(i, 2))
        return carry

    lax.fori_loop(0, chunks, first, 0)
    pl.semaphore_wait(barrier, 2 + flag(z > 0) + flag(z < CHIPS_Z - 1))

    def body(step, carry):
        @pl.when(step >= RING)
        def _():
            retire(step - RING)

        def stage(i, carry):
            k = STAGES - i
            unit = step - LAG0 - LAG * k

            @pl.when((unit >= 0) & (unit < units))
            def _():
                r = role(unit, y, z)

                @pl.when(r["level"] == k)
                def _():
                    climb(unit, r)

                @pl.when(r["down"] == k)
                def _():
                    descend(unit, r)

            return carry

        lax.fori_loop(0, STAGES + 1, stage, 0)

        @pl.when(step < units)
        def _():
            compute(step)

        return carry

    lax.fori_loop(0, units + RING, body, 0)


def solution(mesh):
    def body(a, g):
        a, g = a[0], g[0]
        matrices, tokens, d = a.shape
        ff = g.shape[2]
        rows = d // (2 * SPLIT)
        block = (rows, COLS)
        dma = pltpu.SemaphoreType.DMA
        flops = 2 * matrices * tokens * d * ff
        return pl.pallas_call(
            kernel,
            out_shape=jax.ShapeDtypeStruct((matrices, d, ff), jnp.bfloat16),
            in_specs=[pl.BlockSpec(memory_space=pl.ANY)] * 2,
            out_specs=pl.BlockSpec(memory_space=pl.ANY),
            scratch_shapes=[
                pltpu.VMEM((2, d, tokens), jnp.bfloat16),
                pltpu.VMEM((2, A_STEP, d), jnp.bfloat16),
                pltpu.VMEM((3, tokens, COLS), jnp.bfloat16),
                pltpu.VMEM((2 * rows, COLS), jnp.float32),
                pltpu.VMEM((SUMS, *block), jnp.float32),
                pltpu.VMEM((RING, *block), jnp.bfloat16),
                pltpu.VMEM((4, RING, *block), jnp.bfloat16),
                pltpu.VMEM((RING, *block), jnp.bfloat16),
                dma((2,)),
                dma((3,)),
                dma((RING,)),
                dma((4, RING)),
                dma((RING,)),
                dma((RING,)),
                dma((5, RING)),
                dma((RING,)),
            ],
            compiler_params=pltpu.CompilerParams(
                collective_id=0, has_side_effects=True, vmem_limit_bytes=67_043_328
            ),
            cost_estimate=pl.CostEstimate(
                flops=flops, bytes_accessed=2 * matrices * (tokens + d) * (d + ff), transcendentals=0
            ),
        )(a, g)

    spec = P(("rep", "dp"))
    return jax.shard_map(body, mesh=mesh, in_specs=(spec, spec), out_specs=P("rep"), check_vma=False)
```

```python
import jax
import jax.numpy as jnp
from jax import lax
from jax.experimental import pallas as pl
from jax.experimental.pallas import tpu as pltpu
from jax.sharding import PartitionSpec as P

MESH = pl.DeviceIdType.MESH
CHIPS_Z = 4
LEFT, RIGHT, ACROSS, PAIR = range(4)

PANELS = 2
COLS = 256
A_STEP = 256
A_SLOTS = 8
LAG0 = 2
LAG = 4
STAGES = 8
RING = LAG0 + LAG * STAGES + 3
QUEUE = 4
SUMS = LAG0 + LAG * (STAGES // 2) + 1


TREES = (
    (1, 2, 1), (0, 3, 0), (0, 0, 0), (1, 2, 1), (1, 1, 0),
    (0, 1, 0), (1, 2, 0), (0, 2, 1), (1, 1, 0), (1, 2, 1),
)


FLAGS = "root", "up_right", "up_left", "up_across", "from_left", "from_right", "from_across"
UP, DOWN = 1, 2


def flag(condition):
    return jnp.where(condition, jnp.int32(1), jnp.int32(0))


def div(x, by):
    return lax.div(x, jnp.int32(by))


def role(tree, y, z):
    across_first, root_z, root_y = tree
    below, above, same = z < root_z, z > root_z, z == root_z
    home = y == root_y
    height = max(root_z, 3 - root_z) + 1
    along = jnp.where(below, z, 3 - z)
    if across_first:
        level = jnp.where(home, jnp.where(same, height, 1 + along), 0)
        in_line, crosses = home, y >= 0
    else:
        level = jnp.where(same, jnp.where(home, height, height - 1), along)
        in_line, crosses = y >= 0, same
    down = height + jnp.abs(z - root_z) + flag(~home)
    flags = (
        home & same,
        in_line & below,
        in_line & above,
        ~home & crosses,
        in_line & (z <= root_z) & (z > 0),
        in_line & (z >= root_z) & (z < CHIPS_Z - 1),
        home & crosses,
    )
    return level, down, [flag(f) for f in flags]


def kernel(
    a_hbm, g_hbm, out_hbm,
    roles, plan, a_t, a_in, g_in, sums, outgoing, arrived, final,
    a_sem, g_sem, outgoing_sem, arrived_sem, climb_sem, final_sem, leave_sem, other_sem,
):
    matrices, tokens, d = a_hbm.shape
    ff = g_hbm.shape[2]
    rows = d // (2 * PANELS)
    steps = ff // COLS
    panels = matrices * PANELS
    units = panels * steps
    chunks = tokens // A_STEP

    rep, me = lax.axis_index("rep"), lax.axis_index("dp")
    core = lax.rem(me, 2)
    chip = div(me, 2)
    z = lax.rem(chip, CHIPS_Z)
    y = div(chip, CHIPS_Z)
    partner = me + 1 - 2 * core
    across = me + 2 * CHIPS_Z * (1 - 2 * y)

    def device(i):
        return (rep, i)

    barrier = pltpu.get_barrier_semaphore()

    def greet(i):
        pl.semaphore_signal(barrier, inc=1, device_id=device(i), device_id_type=MESH)

    greet(partner)
    greet(across)

    @pl.when(z > 0)
    def _():
        greet(me - 2)

    @pl.when(z < CHIPS_Z - 1)
    def _():
        greet(me + 2)

    def a_copy(panel, i, slot):
        n = div(panel, PANELS)
        row = pl.multiple_of(i * A_STEP, A_STEP)
        column = pl.multiple_of((panel - n * PANELS) * (2 * rows), 2 * rows)
        return pltpu.make_async_copy(
            a_hbm.at[n, pl.ds(row, A_STEP), pl.ds(column, 2 * rows)], a_in.at[slot], a_sem.at[slot]
        )

    def g_copy(unit):
        panel = div(unit, steps)
        n = div(panel, PANELS)
        column = pl.multiple_of((unit - panel * steps) * COLS, COLS)
        slot = lax.rem(unit, 3)
        return pltpu.make_async_copy(g_hbm.at[n, :, pl.ds(column, COLS)], g_in.at[slot], g_sem.at[slot])

    def transpose(panel, i, slot):
        a_t[lax.rem(panel, 2), :, pl.ds(pl.multiple_of(i * A_STEP, A_STEP), A_STEP)] = a_in[slot].T

    def place(unit, of_core):
        panel = div(unit, steps)
        n = div(panel, PANELS)
        row = pl.multiple_of((panel - n * PANELS) * (2 * rows) + of_core * rows, rows)
        column = pl.multiple_of((unit - panel * steps) * COLS, COLS)
        return out_hbm.at[n, pl.ds(row, rows), pl.ds(column, COLS)]

    def fetch_first(i, slot):
        a_copy(jnp.int32(0), i, slot).start()

    for i in range(min(A_SLOTS, chunks)):
        fetch_first(i, i)
    g_copy(jnp.int32(0)).start()
    g_copy(jnp.int32(1)).start()

    turns = len(TREES)
    places = [role(tree, y, z) for tree in TREES]
    for turn, (_, _, flags) in enumerate(places):
        for i, value in enumerate(flags):
            roles[turn, i] = value
    for turn in range(turns):
        for k in range(STAGES + 1):
            level, down, _ = places[(turn - LAG0 - LAG * k) % turns]
            plan[turn, k] = UP * flag(level == k) + DOWN * flag(down == k)

    def role_of(unit):
        turn = lax.rem(unit, turns)
        return {name: roles[turn, i] == 1 for i, name in enumerate(FLAGS)}

    def slot_of(unit):
        return lax.rem(unit, RING)

    def pair_copy(unit):
        slot, queue = slot_of(unit), lax.rem(unit, QUEUE)
        return pltpu.make_async_remote_copy(
            src_ref=outgoing.at[queue], dst_ref=arrived.at[PAIR, slot],
            send_sem=outgoing_sem.at[queue], recv_sem=arrived_sem.at[PAIR, slot],
            device_id=device(partner), device_id_type=MESH,
        )

    def climb_copy(unit, side, to):
        slot = slot_of(unit)
        return pltpu.make_async_remote_copy(
            src_ref=arrived.at[PAIR, slot], dst_ref=arrived.at[side, slot],
            send_sem=climb_sem.at[slot], recv_sem=arrived_sem.at[side, slot],
            device_id=device(to), device_id_type=MESH,
        )

    def final_copy(unit, side, to):
        slot = slot_of(unit)
        return pltpu.make_async_remote_copy(
            src_ref=final.at[slot], dst_ref=final.at[slot],
            send_sem=leave_sem.at[side, slot], recv_sem=final_sem.at[slot],
            device_id=device(to), device_id_type=MESH,
        )

    def other_copy(unit, of_core):
        slot = slot_of(unit)
        return pltpu.make_async_remote_copy(
            src_ref=final.at[slot], dst_ref=place(unit, of_core),
            send_sem=leave_sem.at[PAIR, slot], recv_sem=other_sem.at[slot],
            device_id=device(partner), device_id_type=MESH,
        )

    def own_copy(unit):
        slot = slot_of(unit)
        return pltpu.make_async_copy(final.at[slot], place(unit, core), leave_sem.at[4, slot])

    def compute(unit):
        panel = div(unit, steps)
        step = unit - panel * steps

        @pl.when(unit + 2 < units)
        def _():
            g_copy(unit + 2).start()

        g_copy(unit).wait()
        at = lax.rem(unit, SUMS)
        sums[at] = jnp.dot(a_t[lax.rem(panel, 2)], g_in[lax.rem(unit, 3)], preferred_element_type=jnp.float32)
        outgoing[lax.rem(unit, QUEUE)] = sums[at, pl.ds(pl.multiple_of((1 - core) * rows, rows), rows), :].astype(jnp.bfloat16)
        pair_copy(unit).start()

        @pl.when(panel < panels - 1)
        def _():
            @pl.when(step < chunks)
            def _():
                a_copy(panel + 1, step, lax.rem(step, A_SLOTS)).start()

            @pl.when((step >= 1) & (step <= chunks))
            def _():
                i = step - 1
                a_copy(panel + 1, i, lax.rem(i, A_SLOTS)).wait()
                transpose(panel + 1, i, lax.rem(i, A_SLOTS))

    def climb(unit, r):
        slot = slot_of(unit)
        own = sums.at[lax.rem(unit, SUMS), pl.ds(pl.multiple_of(core * rows, rows), rows), :]
        for side, there, source in (
            (LEFT, r["from_left"], me - 2),
            (RIGHT, r["from_right"], me + 2),
            (ACROSS, r["from_across"], across),
        ):
            @pl.when(there)
            def _():
                climb_copy(unit, side, source).wait_recv()
                own[...] = own[...] + arrived[side, slot].astype(jnp.float32)

        pair_copy(unit).wait_recv()
        total = (own[...] + arrived[PAIR, slot].astype(jnp.float32)).astype(jnp.bfloat16)

        @pl.when(r["root"])
        def _():
            final[slot] = total

        @pl.when(~r["root"])
        def _():
            arrived[PAIR, slot] = total

        for side, there, to in (
            (LEFT, r["up_right"], me + 2),
            (RIGHT, r["up_left"], me - 2),
            (ACROSS, r["up_across"], across),
        ):
            @pl.when(there)
            def _():
                climb_copy(unit, side, to).start()

    def children(unit, r, act):
        for side, there, to in (
            (LEFT, r["from_left"], me - 2),
            (RIGHT, r["from_right"], me + 2),
            (ACROSS, r["from_across"], across),
        ):
            @pl.when(there)
            def _():
                act(final_copy(unit, side, to))

    def descend(unit, r):
        @pl.when(~r["root"])
        def _():
            climb_copy(unit, LEFT, partner).wait_send()
            final_copy(unit, LEFT, partner).wait_recv()

        children(unit, r, lambda copy: copy.start())
        other_copy(unit, core).start()
        own_copy(unit).start()

    def retire(unit):
        r = role_of(unit)
        children(unit, r, lambda copy: copy.wait_send())
        other_copy(unit, core).wait_send()
        own_copy(unit).wait()
        other_copy(unit, 1 - core).wait_recv()

    def first(i, carry):
        slot = lax.rem(i, A_SLOTS)
        a_copy(jnp.int32(0), i, slot).wait()
        transpose(jnp.int32(0), i, slot)

        @pl.when(i + A_SLOTS < chunks)
        def _():
            fetch_first(i + A_SLOTS, slot)

        return carry

    lax.fori_loop(0, chunks, first, 0)
    pl.semaphore_wait(barrier, 2 + flag(z > 0) + flag(z < CHIPS_Z - 1))

    def body(step, carry):
        @pl.when(step >= RING)
        def _():
            retire(step - RING)

        turn = lax.rem(step, turns)

        def stage(i, carry):
            k = STAGES - i
            unit = step - LAG0 - LAG * k
            what = plan[turn, k]

            @pl.when((what > 0) & (unit >= 0) & (unit < units))
            def _():
                r = role_of(unit)

                @pl.when(what != DOWN)
                def _():
                    climb(unit, r)

                @pl.when(what >= DOWN)
                def _():
                    descend(unit, r)

            return carry

        lax.fori_loop(0, STAGES + 1, stage, 0)

        @pl.when((step >= QUEUE) & (step < units + QUEUE))
        def _():
            pair_copy(step - QUEUE).wait_send()

        @pl.when(step < units)
        def _():
            compute(step)

        return carry

    lax.fori_loop(0, units + RING, body, 0)


HAND_SLOTS, HAND_LEAD, HAND_ROWS = 16, 8, 128


def hand_over(x_hbm, out_hbm, held, in_sem, out_sem):
    matrices, d, _ = x_hbm.shape
    pieces = [(n, pl.ds(row, HAND_ROWS)) for n in range(matrices) for row in range(0, d, HAND_ROWS)]

    def take(i):
        slot = i % HAND_SLOTS
        return pltpu.make_async_copy(x_hbm.at[pieces[i]], held.at[slot], in_sem.at[slot])

    def give(i):
        slot = i % HAND_SLOTS
        return pltpu.make_async_copy(held.at[slot], out_hbm.at[pieces[i]], out_sem.at[slot])

    for i in range(min(HAND_SLOTS, len(pieces))):
        take(i).start()
    for i in range(len(pieces) + HAND_LEAD):
        if i < len(pieces):
            take(i).wait()
            give(i).start()
        if i >= HAND_LEAD:
            give(i - HAND_LEAD).wait()
            if i - HAND_LEAD + HAND_SLOTS < len(pieces):
                take(i - HAND_LEAD + HAND_SLOTS).start()


def solution(mesh):
    def body(a, g):
        a, g = a[0], g[0]
        matrices, tokens, d = a.shape
        ff = g.shape[2]
        rows = d // (2 * PANELS)
        block = (rows, COLS)
        dma = pltpu.SemaphoreType.DMA
        flops = 2 * matrices * tokens * d * ff
        sums = pl.pallas_call(
            kernel,
            out_shape=jax.ShapeDtypeStruct((matrices, d, ff), jnp.bfloat16),
            in_specs=[pl.BlockSpec(memory_space=pl.ANY)] * 2,
            out_specs=pl.BlockSpec(memory_space=pl.ANY),
            scratch_shapes=[
                pltpu.SMEM((len(TREES), len(FLAGS)), jnp.int32),
                pltpu.SMEM((len(TREES), STAGES + 1), jnp.int32),
                pltpu.VMEM((2, 2 * rows, tokens), jnp.bfloat16),
                pltpu.VMEM((A_SLOTS, A_STEP, 2 * rows), jnp.bfloat16),
                pltpu.VMEM((3, tokens, COLS), jnp.bfloat16),
                pltpu.VMEM((SUMS, 2 * rows, COLS), jnp.float32),
                pltpu.VMEM((QUEUE, *block), jnp.bfloat16),
                pltpu.VMEM((4, RING, *block), jnp.bfloat16),
                pltpu.VMEM((RING, *block), jnp.bfloat16),
                dma((A_SLOTS,)),
                dma((3,)),
                dma((QUEUE,)),
                dma((4, RING)),
                dma((RING,)),
                dma((RING,)),
                dma((5, RING)),
                dma((RING,)),
            ],
            compiler_params=pltpu.CompilerParams(
                collective_id=0, has_side_effects=True, vmem_limit_bytes=67_043_328
            ),
            cost_estimate=pl.CostEstimate(
                flops=flops, bytes_accessed=2 * matrices * (tokens + d) * (d + ff), transcendentals=0
            ),
        )(a, g)
        return pl.pallas_call(
            hand_over,
            out_shape=jax.ShapeDtypeStruct(sums.shape, sums.dtype),
            in_specs=[pl.BlockSpec(memory_space=pl.ANY)],
            out_specs=pl.BlockSpec(memory_space=pl.ANY),
            scratch_shapes=[pltpu.VMEM((HAND_SLOTS, HAND_ROWS, ff), sums.dtype), dma((HAND_SLOTS,)), dma((HAND_SLOTS,))],
        )(sums)

    spec = P(("rep", "dp"))
    return jax.shard_map(body, mesh=mesh, in_specs=(spec, spec), out_specs=P("rep"), check_vma=False)
```
